32 devices in a mesh: seq: 16 (over z, y, x), tp: 2 (over core).
Axes of the slice: x: 2, y: 2, z: 4, core: 2. Of those that a mesh axis runs over, the one named last changes fastest.
Arguments:
- img_qkv: bfloat16 [1, 512, 3, 2048], P(None, 'seq', None, 'tp'), may hold values from -7 to 7
- txt_qkv: bfloat16 [1, 256, 3, 2048], P(None, None, None, 'tp'), may hold values from -7 to 7
- frame_index: int32 [1, 512], P(None, 'seq'), may hold values from 0 to 32
- row_index: int32 [1, 512], P(None, 'seq'), may hold values from 0 to 44
- column_index: int32 [1, 512], P(None, 'seq'), may hold values from 0 to 79
- txt_len: int32 [1], replicated, may hold values from 64 to 256
- residual: bfloat16 [1, 512, 3072], P(None, ('seq', 'tp')), may hold values from -6 to 6
- w_proj: bfloat16 [2048, 3072], P('tp'), may hold values from -0.125 to 0.125
- proj_bias: float32 [3072], replicated, may hold values from -3 to 3
- gate: float32 [3072], replicated, may hold values from -4 to 4
Outputs:
- img_out: bfloat16 [1, 512, 3072], P(None, ('seq', 'tp'))
- txt_out: bfloat16 [1, 256, 2048], P(None, None, 'tp')
The draws below stay inside these ranges and needn't reach their ends.
All inputs are finite; a program needn't handle non-finite values.
Results may differ from the reference program's by a relative error of at most 0.0082.
Values may be sent and summed in bfloat16 or wider, within the bound.
A program may use at most 64 MiB of HBM per device.

```python
import math
import jax
import jax.numpy as jnp
from jax import lax

D = 3072
HD = 128
HEADS = 16
TXT = 256
LAT_T = 33
LAT_H = 45
LAT_W = 80
CLIPS = 1
IMG = 512
QW = 2048


def draw_img_qkv(key, part):
    width_all = HEADS * HD
    total_rows = CLIPS * IMG
    subkeys = jax.random.split(jax.random.fold_in(key, 11), 4)
    query_part = jnp.clip(1.8 * jax.random.normal(subkeys[0], (total_rows, width_all), jnp.float32), -7.0, 7.0)
    key_part = jnp.clip(1.8 * jax.random.normal(subkeys[1], (total_rows, width_all), jnp.float32), -7.0, 7.0)
    value_part = jnp.clip(jax.random.normal(subkeys[3], (total_rows, width_all), jnp.float32), -6.0, 6.0)
    stacked = jnp.stack([query_part, key_part, value_part], axis=1)
    return stacked.reshape(CLIPS, IMG, 3, width_all).astype(jnp.bfloat16)


def draw_txt_qkv(key, part):
    width_all = HEADS * HD
    subkeys = jax.random.split(jax.random.fold_in(key, 23), 4)
    query_part = jnp.clip(1.8 * jax.random.normal(subkeys[0], (CLIPS, TXT, width_all), jnp.float32), -7.0, 7.0)
    key_part = jnp.clip(1.8 * jax.random.normal(subkeys[1], (CLIPS, TXT, width_all), jnp.float32), -7.0, 7.0)
    value_part = jnp.clip(jax.random.normal(subkeys[3], (CLIPS, TXT, width_all), jnp.float32), -6.0, 6.0)
    return jnp.stack([query_part, key_part, value_part], axis=2).astype(jnp.bfloat16)


def plant(values, own_key, low, high):
    extent = values.shape
    index_at = [jax.random.randint(jax.random.fold_in(own_key, axis), (), 0, extent[axis]) for axis in range(len(extent))]
    values = values.at[tuple(index_at)].set(low)
    longest = extent.index(max(extent))
    index_at[longest] = (index_at[longest] + 1) % extent[longest]
    return values.at[tuple(index_at)].set(high)


def steps_of(key, dims, cuts, least, high):
    def one(dim, parts):
        steps = jax.random.uniform(jax.random.fold_in(jax.random.fold_in(key, 6), dim), (parts,), jnp.float32, least / len(cuts), high / len(cuts))
        return jnp.repeat(jnp.exp(steps), dims[dim] // parts).reshape((-1,) + (1,) * (len(dims) - dim - 1))

    factor_of = one(*cuts[0])
    for cut in cuts[1:]:
        factor_of = factor_of * one(*cut)
    return factor_of


def normal_values(rng, shape, scale, limit, cuts=(), held_as=jnp.bfloat16):
    values = scale * jax.random.normal(rng, shape, jnp.float32)
    if cuts:
        values = values * steps_of(rng, shape, cuts, -0.22, 0.18)
    return jnp.clip(values, -limit, limit).astype(held_as)


def setup_inputs(seed: int = 0) -> dict:
    seeds = jax.random.split(jax.random.key(seed), 11)
    img_qkv = draw_img_qkv(jax.random.fold_in(seeds[10], 71), 0)
    txt_qkv = draw_txt_qkv(jax.random.fold_in(seeds[10], 71), 0)
    frame_index = plant(jax.random.randint(seeds[2], (CLIPS, IMG), 0, LAT_T), jax.random.fold_in(seeds[2], 1), 0, LAT_T - 1).astype(jnp.int32)
    row_index = plant(jax.random.randint(seeds[3], (CLIPS, IMG), 0, LAT_H), jax.random.fold_in(seeds[3], 1), 0, LAT_H - 1).astype(jnp.int32)
    column_index = plant(jax.random.randint(seeds[4], (CLIPS, IMG), 0, LAT_W), jax.random.fold_in(seeds[4], 1), 0, LAT_W - 1).astype(jnp.int32)
    txt_len = jax.random.randint(seeds[5], (CLIPS,), TXT // 4, TXT + 1).astype(jnp.int32)
    residual = normal_values(seeds[6], (CLIPS, IMG, D), 1.0, 6.0, ((1, 32),))
    w_proj = normal_values(seeds[7], (QW, D), QW ** -0.5, 0.125, ((0, 2),))
    proj_bias = normal_values(seeds[8], (D,), 0.5, 3.0, (), jnp.float32)
    gate = normal_values(seeds[9], (D,), 1.0, 4.0, (), jnp.float32)
    return {"img_qkv": img_qkv, "txt_qkv": txt_qkv, "frame_index": frame_index, "row_index": row_index, "column_index": column_index, "txt_len": txt_len, "residual": residual, "w_proj": w_proj, "proj_bias": proj_bias, "gate": gate}


rope_base = 256.0
neg_large = -1e+30

def rope_tables(frame_index, row_index, column_index, head_dim):
    frame_part = head_dim // 8
    second = (head_dim - frame_part) // 2
    pieces = []
    for places, part_width in ((frame_index, frame_part), (row_index, second), (column_index, second)):
        pair_ids = jnp.arange(part_width // 2).astype(jnp.float32)
        pair_rates = rope_base ** (-2.0 * pair_ids / part_width)
        pieces.append(places.astype(jnp.float32)[:, None] * pair_rates[None, :])
    angles = jnp.repeat(jnp.concatenate(pieces, axis=1), 2, axis=1)
    parity = jnp.arange(head_dim) % 2
    signed = jnp.where(parity == 0, -1.0, 1.0).astype(jnp.float32)
    return (jnp.cos(angles), jnp.sin(angles) * signed[None, :])

def rotate(block_in, cosine, sine_table):
    values = block_in.astype(jnp.float32)
    parity = jnp.arange(values.shape[-1]) % 2
    partner = jnp.where(parity == 0, jnp.roll(values, -1, axis=-1), jnp.roll(values, 1, axis=-1))
    return (values * cosine[:, None, :] + partner * sine_table[:, None, :]).astype(jnp.bfloat16)

def attend_head(query_head, key_head, value_head, live_keys):
    row_count = query_head.shape[0]
    row_block = 1
    for candidate in range(1, 1025):
        if row_count % candidate == 0:
            row_block = candidate
    blocks = query_head.reshape(row_count // row_block, row_block, query_head.shape[1])
    score_scale = 1.0 / math.sqrt(query_head.shape[1])

    def one_block(query_block):
        scores = jnp.dot(query_block, key_head.T, preferred_element_type=jnp.float32) * score_scale
        scores = jnp.where(live_keys[None, :], scores, neg_large)
        peak = lax.optimization_barrier(jnp.max(scores, axis=1, keepdims=True))
        weights = jnp.where(live_keys[None, :], jnp.exp(scores - peak), 0.0)
        weight_sum = lax.optimization_barrier(jnp.sum(weights, axis=1, keepdims=True))
        blended = jnp.dot(weights.astype(jnp.bfloat16), value_head, preferred_element_type=jnp.float32)
        return (blended / weight_sum).astype(jnp.bfloat16)
    return lax.map(one_block, blocks).reshape(row_count, query_head.shape[1])

def clip_attention(clip_qkv, clip_txt, frames, rows_at, columns_at, length):
    cosine, sine_table = rope_tables(frames, rows_at, columns_at, HD)
    img_query = rotate(clip_qkv[:, 0].reshape(IMG, HEADS, HD), cosine, sine_table)
    img_key = rotate(clip_qkv[:, 1].reshape(IMG, HEADS, HD), cosine, sine_table)
    img_value = clip_qkv[:, 2].reshape(IMG, HEADS, HD)
    queries = jnp.concatenate([img_query, clip_txt[:, 0].reshape(TXT, HEADS, HD)], axis=0)
    all_keys = jnp.concatenate([img_key, clip_txt[:, 1].reshape(TXT, HEADS, HD)], axis=0)
    all_values = jnp.concatenate([img_value, clip_txt[:, 2].reshape(TXT, HEADS, HD)], axis=0)
    live_keys = jnp.arange(IMG + TXT) < IMG + length

    def head_work(operands):
        return attend_head(operands[0], operands[1], operands[2], live_keys)
    attended = lax.map(head_work, (queries.transpose(1, 0, 2), all_keys.transpose(1, 0, 2), all_values.transpose(1, 0, 2)))
    joined = attended.transpose(1, 0, 2).reshape(IMG + TXT, HEADS * HD)
    img_rows = joined[:IMG]
    txt_rows = joined[IMG:]
    txt_live = jnp.arange(TXT) < length
    txt_rows = jnp.where(txt_live[:, None], txt_rows, jnp.zeros_like(txt_rows))
    return (img_rows, txt_rows)

def reference(img_qkv, txt_qkv, frame_index, row_index, column_index, txt_len, residual, w_proj, proj_bias, gate):
    img_outs = []
    txt_outs = []
    for clip in range(CLIPS):
        img_rows, txt_rows = clip_attention(img_qkv[clip], txt_qkv[clip], frame_index[clip], row_index[clip], column_index[clip], txt_len[clip])
        projected = jnp.dot(img_rows, w_proj, preferred_element_type=jnp.float32)
        mixed = residual[clip].astype(jnp.float32) + gate[None, :] * (projected + proj_bias[None, :])
        img_outs.append(mixed.astype(jnp.bfloat16))
        txt_outs.append(txt_rows)
    return (jnp.stack(img_outs, axis=0), jnp.stack(txt_outs, axis=0))
```

```python
import functools
import math

import jax
import jax.numpy as jnp
from jax import lax
from jax.experimental import pallas as pl
from jax.experimental.pallas import tpu as pltpu
from jax.sharding import PartitionSpec as P

HD = 128
ROPE_BASE_LOG2 = 8.0
NEG_LARGE = -1e30
F32 = jnp.float32
BF16 = jnp.bfloat16
LOADS = 11
DIRECT = (0, 1, 2, 3)


def largest_divisor(n):
    best = 1
    for d in range(1, n + 1):
        if n % d == 0 and d * d <= n:
            best = d
    return best


def over(start, count, f):
    if count - start <= 8:
        for o in range(start, count):
            f(o)
    else:
        lax.fori_loop(start, count, lambda o, c: (f(o), c)[1], 0)


class Ring:
    def __init__(self, index, count):
        self.index, self.count = index, count
        self.paired = count & (count - 1) == 0
        self.flips = []
        if self.paired:
            bit = 1
            while bit < count:
                self.flips.append((bit, (1 - 2 * ((index // bit) % 2)) * bit))
                bit *= 2

    def meet(self, o, sign):
        if not self.paired:
            return (self.index + sign * o + self.count) % self.count
        total = self.index
        for bit, flip in self.flips:
            if isinstance(o, int):
                total = total + flip if o & bit else total
            else:
                total = total + flip * ((o // bit) % 2)
        return total

    def to(self, o):
        return self.meet(o, 1)

    def source(self, o):
        return self.meet(o, -1)


def kernel(
    n, heads, img_hbm, txt_hbm, frame_hbm, row_hbm, column_hbm, len_ref, res_hbm, w_hbm, bias_hbm, gate_hbm,
    out_ref, txt_out,
    img_ref, txt_q, places, q_send, k_send, q_all, k_all, v_all, a_send, home, t_send, w, res, bias, gate, total, p_send,
    p_recv, load_sem, k_ss, v_ss, q_ss, kr_ss, vr_ss, a_ss, p_ss, t_ss, k_rs, v_rs, q_rs, kr_rs, vr_rs, a_rs, t1_rs, t2_rs,
    t3_rs, p_rs,
):
    p = lax.axis_index("seq")
    t = lax.axis_index("tp")
    groups = n // heads
    head = p // groups
    group = p % groups
    tokens = img_ref.shape[1]
    text = txt_hbm.shape[1]
    share = text // groups
    plane_keys = heads * tokens
    early_keys = plane_keys + text
    scale = 1.0 / math.sqrt(HD)
    chunks = p_send.shape[0]
    width = p_send.shape[2]
    half = tokens // 2
    plane = largest_divisor(n)
    lines = n // plane
    inner = largest_divisor(plane)
    outer = plane // inner
    line = p // plane
    v = p % inner
    u = (p // inner) % outer
    direct = [o for o in DIRECT if o < lines]
    near = plane % groups == 0 and groups % inner == 0 and inner % groups == 0
    by_head, by_group = Ring(head, heads), Ring(group, groups)
    by_line, by_u, by_v = Ring(line, lines), Ring(u, outer), Ring(v, inner)
    joined = 2 if by_head.paired and heads % 2 == 0 else heads
    pairs = heads // joined
    by_pair = Ring(head // joined, pairs)

    def rows(first, count):
        return pl.ds(pl.multiple_of(first, count), count)

    def cols(h):
        return pl.ds(pl.multiple_of(h * HD, HD), HD)

    def plane_slot(j):
        return rows(j * tokens, tokens)

    def relay_slot(o, j):
        return pl.ds(pl.multiple_of(early_keys + ((o - 1) * heads + j) * tokens, tokens), tokens)

    def remote(src, dst, send, recv, where):
        return pltpu.make_async_remote_copy(src, dst, send, recv, device_id=where)

    barrier = pltpu.get_barrier_semaphore()

    def greet(where):
        pl.semaphore_signal(barrier, inc=1, device_id=where)

    if near:
        over(1, heads, lambda o: greet({"seq": by_head.to(heads - o) * groups + group}))
        over(1, groups, lambda o: greet({"seq": head * groups + by_group.to(o)}))
        greetings = heads + groups - 1
        if direct:
            for i in range(1, outer):
                over(1, inner, lambda o, i=i: greet({"seq": line * plane + by_u.to(i) * inner + by_v.to(o)}))
            greetings += (outer - 1) * (inner - 1)
    else:
        over(1, n, lambda o: greet({"seq": (p + o) % n}))
        greetings = n
    greet({"tp": 1 - t})

    own_text = rows(group * share, share)
    text_keys = pl.ds(plane_keys, text)
    loads = [
        pltpu.make_async_copy(src, dst, load_sem.at[i])
        for i, (src, dst) in enumerate(
            (
                (frame_hbm, places.at[0]),
                (row_hbm, places.at[1]),
                (column_hbm, places.at[2]),
                (img_hbm, img_ref),
                (txt_hbm.at[0, own_text, cols(head)], txt_q),
                (txt_hbm.at[1, :, cols(head)], k_all.at[text_keys]),
                (txt_hbm.at[2, :, cols(head)], v_all.at[text_keys]),
                (w_hbm, w),
                (res_hbm, res),
                (bias_hbm, bias),
                (gate_hbm, gate),
            )
        )
    ]
    for load in loads:
        load.start()

    diagonal = lax.broadcasted_iota(jnp.int32, (tokens, tokens), 0) == lax.broadcasted_iota(
        jnp.int32, (tokens, tokens), 1
    )
    channel = lax.broadcasted_iota(jnp.int32, (1, HD), 1)
    first = HD // 8
    second = (HD - first) // 2
    angles = jnp.zeros((tokens, HD), F32)
    for load in loads[:4]:
        load.wait()
    for part, (start, size) in enumerate(
        ((0, first), (first, second), (first + second, second))
    ):
        inside = (channel >= start) & (channel < start + size)
        pair = ((channel - start) // 2).astype(F32)
        rate = jnp.where(inside, jnp.exp2(pair * (-2.0 * ROPE_BASE_LOG2 / size)), 0.0)
        column = jnp.sum(
            jnp.where(diagonal, places[part].astype(F32), 0.0), axis=1, keepdims=True
        )
        angles = angles + column * rate
    even = lax.broadcasted_iota(jnp.int32, (tokens, HD), 1) % 2 == 0
    cosine = jnp.cos(angles)
    sine = jnp.where(even, -1.0, 1.0) * jnp.sin(angles)
    for which, dst in ((1, k_send), (0, q_send)):
        for h in range(heads):
            x = img_ref[which, :, h * HD : (h + 1) * HD].astype(F32)
            partner = jnp.where(even, pltpu.roll(x, HD - 1, 1), pltpu.roll(x, 1, 1))
            dst[h] = (x * cosine + partner * sine).astype(BF16)
    k_all[plane_slot(head), :] = k_send[head]
    v_all[plane_slot(head), :] = img_ref[2, :, cols(head)]
    q_all[plane_slot(head), :] = q_send[head]

    pl.semaphore_wait(barrier, greetings)

    def line_up(h):
        return {"seq": h * groups + group}

    def k_copy(o, h, j):
        return remote(k_send.at[h], k_all.at[plane_slot(j)], k_ss, k_rs.at[o], line_up(h))

    def v_copy(o, h, j):
        return remote(img_ref.at[2, :, cols(h)], v_all.at[plane_slot(j)], v_ss, v_rs.at[o], line_up(h))

    def q_copy(h):
        return remote(q_send.at[h], q_all.at[plane_slot(head)], q_ss, q_rs, line_up(h))

    def relay(data, send, recv, j):
        def one(o):
            g = by_group.to(o)
            remote(
                data.at[plane_slot(j)], data.at[relay_slot(o, j)], send, recv, {"seq": head * groups + g}
            ).start()

        over(1, groups, one)

    def all_of(count, send, recv):
        wide = -(-count // k_all.shape[0])
        block = k_all.at[pl.ds(0, count)] if wide == 1 else w.at[pl.ds(0, count * HD // w.shape[1])]
        return remote(block, block, send, recv, {"tp": 1 - t})

    relay(k_all, kr_ss, kr_rs, head)
    over(1, heads, lambda o: k_copy(o, by_head.to(o), head).start())
    relay(v_all, vr_ss, vr_rs, head)
    over(1, heads, lambda o: v_copy(o, by_head.to(o), head).start())
    over(1, heads, lambda o: q_copy(by_head.to(o)).start())

    def pass_on(copy, data, send, recv):
        def one(o):
            j = by_head.source(o)
            copy(o, head, j).wait_recv()
            relay(data, send, recv, j)

        over(1, heads, one)

    pass_on(k_copy, k_all, kr_ss, kr_rs)
    pass_on(v_copy, v_all, vr_ss, vr_rs)
    for load in loads[4:7]:
        load.wait()
    length = len_ref[0]
    relayed = (groups - 1) * plane_keys

    def scores_of(queries, start, count):
        return lax.dot_general(
            queries, k_all[pl.ds(start, count), :], (((1,), (1,)), ((), ())), preferred_element_type=F32
        )

    def early_scores(queries):
        scores = scores_of(queries, 0, early_keys)
        live = lax.broadcasted_iota(jnp.int32, scores.shape, 1) < plane_keys + length
        return jnp.where(live, scores, NEG_LARGE)

    def weigh(queries, scores):
        peak = jnp.max(scores, axis=1, keepdims=True)
        parts = [scores]
        if relayed:
            parts.append(scores_of(queries, early_keys, relayed))
            peak = jnp.maximum(peak, jnp.max(parts[1], axis=1, keepdims=True))
        live = lax.broadcasted_iota(jnp.int32, scores.shape, 1) < plane_keys + length
        weights = [jnp.exp((part - peak) * scale) for part in parts]
        weights[0] = jnp.where(live, weights[0], 0.0)
        whole = sum(jnp.sum(part, axis=1, keepdims=True) for part in weights)
        return [part.astype(BF16) for part in weights], whole

    def blend(weights, whole):
        mixed = jnp.dot(weights[0], v_all[pl.ds(0, early_keys), :], preferred_element_type=F32)
        if relayed:
            mixed = mixed + jnp.dot(weights[1], v_all[pl.ds(early_keys, relayed), :], preferred_element_type=F32)
        return mixed / whole

    text_scores = early_scores(txt_q[...])
    if heads > 1:
        all_of((heads - 1) * tokens, q_ss, q_rs).wait_recv()
    if relayed:
        all_of(relayed, kr_ss, kr_rs).wait_recv()
    text_weights, text_total = weigh(txt_q[...], text_scores)
    image_weights, image_total = weigh(q_all[...], early_scores(q_all[...]))
    if relayed:
        all_of(relayed, vr_ss, vr_rs).wait_recv()
    text_done = blend(text_weights, text_total)
    text_row = lax.broadcasted_iota(jnp.int32, text_done.shape, 0) + group * share
    text_done = jnp.where(text_row < length, text_done, 0.0).astype(BF16)

    def place(l, uu, vv):
        return l * plane + uu * inner + vv

    def block(s):
        return txt_out.at[rows((s % groups) * share, share), cols(s // groups)]

    def line_copy(o, to, s):
        return remote(t_send, block(s), t_ss.at[0], t1_rs.at[o], {"seq": place(to, u, v)})

    def along(ring, at):
        return [(o, at(ring.to(o)), at(ring.source(o))) for o in range(1, ring.count)]

    along_v = along(by_v, lambda x: (u, x))
    along_u = along(by_u, lambda x: (x, v))

    def cross(o, l, own):
        way = o % 2
        first_way, last_way = ((along_v, along_u), (along_u, along_v))[way]
        s = place(l, u, v)
        source = t_send if own else block(s)
        if o in direct:
            corner = [(0, (by_u.to(i), by_v.to(k)), 0) for i in range(1, outer) for k in range(1, inner)]
            for i, to, _ in first_way + last_way + corner:
                remote(source, block(s), t_ss.at[5], t3_rs.at[2], {"seq": place(line, *to)}).start()
            return
        for i, to, _ in first_way:
            remote(source, block(s), t_ss.at[1 + way], t2_rs.at[o, i], {"seq": place(line, *to)}).start()
        for i, to, _ in last_way:
            remote(source, block(s), t_ss.at[3 + way], t3_rs.at[way], {"seq": place(line, *to)}).start()

    def cross_on(o, l):
        if o in direct:
            return
        way = o % 2
        first_way, last_way = ((along_v, along_u), (along_u, along_v))[way]
        for i, _, origin in first_way:
            s = place(l, *origin)
            remote(block(s), block(s), t_ss.at[1 + way], t2_rs.at[o, i], {"tp": 1 - t}).wait_recv()
            for _, to, _ in last_way:
                remote(block(s), block(s), t_ss.at[3 + way], t3_rs.at[way], {"seq": place(line, *to)}).start()

    t_send[...] = text_done
    txt_out[own_text, cols(head)] = text_done
    over(1, lines, lambda o: line_copy(o, by_line.to(o), p).start())

    a_send[...] = blend(image_weights, image_total).astype(BF16)
    home[:, cols(head)] = a_send[plane_slot(head), :]

    def a_send_to(o):
        j = by_head.to(o)
        remote(a_send.at[plane_slot(j)], home.at[:, cols(head)], a_ss, a_rs.at[o // joined], line_up(j)).start()

    over(1, heads, a_send_to)
    cross(0, line, True)

    def receive_pair(o):
        count = joined * tokens - (tokens if o == 0 else 0)
        if count:
            all_of(count, a_ss, a_rs.at[o]).wait_recv()

    def project(o):
        receive_pair(o)
        at = rows(by_pair.to(o) * joined * HD, joined * HD)
        return [
            jnp.dot(home[:, at], w[at, c * width : (c + 1) * width], preferred_element_type=F32)
            for c in range(chunks)
        ]

    def p_copy(c):
        return remote(p_send.at[c], p_recv.at[c], p_ss, p_rs.at[c], {"tp": 1 - t})

    def step(o):
        if o == 0:
            cross_on(0, line)
        else:
            l = by_line.source(o)
            remote(block(p), block(p), t_ss.at[0], t1_rs.at[o], {"tp": 1 - t}).wait_recv()
            cross(o, l, False)

    def keep(o):
        for c, part in enumerate(project(o)):
            at = slice(c * width, (c + 1) * width)
            total[:, at] = part if o == 0 else total[:, at] + part

    for load in loads[7:]:
        load.wait()
    for o in range(lines):
        step(o)
    for o in range(1, lines):
        cross_on(o, by_line.source(o))
    for o in range(pairs - 1):
        keep(o)
    last = project(pairs - 1)
    mine = []
    for c in range(chunks):
        at = slice(c * width, (c + 1) * width)
        part = last[c] if pairs == 1 else total[:, at] + last[c]
        top, bottom = part[:half], part[half:]
        p_send[c] = jnp.where(t == 0, bottom, top).astype(BF16)
        p_copy(c).start()
        mine.append(jnp.where(t == 0, top, bottom))
    for c in range(chunks):
        at = slice(c * width, (c + 1) * width)
        p_copy(c).wait_recv()
        projected = mine[c] + p_recv[c].astype(F32)
        out_ref[:, at] = (
            res[:, at].astype(F32) + gate[:, at] * (projected + bias[:, at])
        ).astype(BF16)

    def finish(count, sem):
        if count:
            all_of(count, sem, sem).wait_send()

    counts = [sum(o % 2 == way and o not in direct for o in range(lines)) for way in (0, 1)]
    spread = len(direct) * (plane - 1) * share
    if spread:
        all_of(spread, t_ss.at[0], t3_rs.at[2]).wait_recv()
    for way, (one, two) in enumerate(((inner, outer), (outer, inner))):
        if counts[way] and two > 1:
            all_of(counts[way] * one * (two - 1) * share, t_ss.at[0], t3_rs.at[way]).wait_recv()
    finish((heads - 1) * tokens, k_ss)
    finish((heads - 1) * tokens, v_ss)
    finish((heads - 1) * tokens, q_ss)
    finish((heads - 1) * tokens, a_ss)
    finish(relayed, kr_ss)
    finish(relayed, vr_ss)
    finish((lines - 1) * share, t_ss.at[0])
    for way, (one, two) in enumerate(((inner, outer), (outer, inner))):
        finish(counts[way] * (one - 1) * share, t_ss.at[1 + way])
        finish(counts[way] * one * (two - 1) * share, t_ss.at[3 + way])
    finish(spread, t_ss.at[5])
    remote(p_send, p_recv, p_ss, p_rs.at[0], {"tp": 1 - t}).wait_send()


def store(img, txt, img_out, txt_out, store_sem):
    stores = [
        pltpu.make_async_copy(a, b.at[0], store_sem.at[i]) for i, (a, b) in enumerate(((txt, txt_out), (img, img_out)))
    ]
    for put in stores:
        put.start()
    for put in stores:
        put.wait()


def shards(img_qkv, txt_qkv, frame_index, row_index, column_index, txt_len, residual, w_proj, proj_bias, gate):
    tokens = img_qkv.shape[1]
    channels = img_qkv.shape[3]
    heads = channels // HD
    n = lax.axis_size("seq")
    groups = n // heads
    text = txt_qkv.shape[1]
    share = text // groups
    plane = largest_divisor(n)
    lines = n // plane
    inner = largest_divisor(plane)
    outer = plane // inner
    model = w_proj.shape[1]
    half = residual.shape[1]
    chunks = 4
    img = img_qkv[0].transpose(1, 0, 2)
    txt = txt_qkv[0].transpose(1, 0, 2)
    hbm = pl.BlockSpec(memory_space=pltpu.HBM)
    vmem = pl.BlockSpec(memory_space=pltpu.VMEM)
    dma = pltpu.SemaphoreType.DMA
    done = pl.pallas_call(
        functools.partial(kernel, n, heads),
        out_shape=(pltpu.VMEM((half, model), BF16), pltpu.VMEM((text, channels), BF16)),
        in_specs=[hbm] * 5 + [pl.BlockSpec(memory_space=pltpu.SMEM)] + [hbm] * 4,
        out_specs=(vmem, vmem),
        scratch_shapes=[
            pltpu.VMEM((3, tokens, channels), BF16),
            pltpu.VMEM((share, HD), BF16),
            pltpu.VMEM((3, 1, tokens), jnp.int32),
            pltpu.VMEM((heads, tokens, HD), BF16),
            pltpu.VMEM((heads, tokens, HD), BF16),
            pltpu.VMEM((heads * tokens, HD), BF16),
            pltpu.VMEM((n * tokens + text, HD), BF16),
            pltpu.VMEM((n * tokens + text, HD), BF16),
            pltpu.VMEM((heads * tokens, HD), BF16),
            pltpu.VMEM((tokens, channels), BF16),
            pltpu.VMEM((share, HD), BF16),
            pltpu.VMEM(w_proj.shape, BF16),
            pltpu.VMEM((half, model), BF16),
            pltpu.VMEM((1, model), F32),
            pltpu.VMEM((1, model), F32),
            pltpu.VMEM((tokens, model), F32),
            pltpu.VMEM((chunks, half, model // chunks), BF16),
            pltpu.VMEM((chunks, half, model // chunks), BF16),
            dma((LOADS,)),
            dma, dma, dma, dma, dma, dma, dma, dma((6,)),
            dma((heads,)), dma((heads,)), dma, dma, dma,
            dma((heads,)), dma((lines,)), dma((lines, max(inner, outer))), dma((3,)), dma((chunks,)),
        ],
        compiler_params=pltpu.CompilerParams(
            collective_id=0, has_side_effects=True, vmem_limit_bytes=60000000
        ),
    )(
        img, txt, frame_index, row_index, column_index, txt_len, residual[0], w_proj,
        proj_bias[None], gate[None],
    )
    out, txt_out = (pltpu.with_memory_space_constraint(x, pltpu.VMEM) for x in done)
    return pl.pallas_call(
        store,
        out_shape=(
            jax.ShapeDtypeStruct((1,) + out.shape, BF16),
            jax.ShapeDtypeStruct((1,) + txt_out.shape, BF16),
        ),
        in_specs=[vmem, vmem],
        out_specs=(hbm, hbm),
        scratch_shapes=[dma((2,))],
        compiler_params=pltpu.CompilerParams(vmem_limit_bytes=8000000),
    )(out, txt_out)


def solution(mesh):
    in_specs = (
        P(None, "seq", None, "tp"),
        P(None, None, None, "tp"),
        P(None, "seq"),
        P(None, "seq"),
        P(None, "seq"),
        P(),
        P(None, ("seq", "tp"), None),
        P("tp", None),
        P(),
        P(),
    )
    out_specs = (P(None, ("seq", "tp"), None), P(None, None, "tp"))
    return jax.shard_map(shards, mesh=mesh, in_specs=in_specs, out_specs=out_specs, check_vma=False)
```

```python
import functools
import math

import jax
import jax.numpy as jnp
from jax import lax
from jax.experimental import pallas as pl
from jax.experimental.pallas import tpu as pltpu
from jax.sharding import PartitionSpec as P

HD = 128
ROPE_BASE_LOG2 = 8.0
NEG_LARGE = -1e30
F32 = jnp.float32
BF16 = jnp.bfloat16
LOADS = 11
HELP, WORK = 0, 1


def largest_divisor(n):
    best = 1
    for d in range(1, n + 1):
        if n % d == 0 and d * d <= n:
            best = d
    return best


def over(start, count, f):
    if count - start <= 8:
        for o in range(start, count):
            f(o)
    else:
        lax.fori_loop(start, count, lambda o, c: (f(o), c)[1], 0)


class Ring:
    def __init__(self, index, count):
        self.index, self.count = index, count
        self.paired = count & (count - 1) == 0
        self.flips = []
        if self.paired:
            bit = 1
            while bit < count:
                self.flips.append((bit, (1 - 2 * ((index // bit) % 2)) * bit))
                bit *= 2

    def meet(self, o, sign):
        if not self.paired:
            return (self.index + sign * o + self.count) % self.count
        total = self.index
        for bit, flip in self.flips:
            if isinstance(o, int):
                total = total + flip if o & bit else total
            else:
                total = total + flip * ((o // bit) % 2)
        return total

    def to(self, o):
        return self.meet(o, 1)

    def source(self, o):
        return self.meet(o, -1)


def kernel(
    n, heads, img_hbm, txt_hbm, frame_hbm, row_hbm, column_hbm, len_ref, res_hbm, w_hbm, bias_hbm, gate_hbm,
    out_ref, txt_out,
    img_ref, txt_q, places, q_send, k_send, q_all, k_all, v_all, a_send, home, t_send, stage, w, res, bias, gate, total,
    p_send, p_recv, load_sem, k_ss, v_ss, q_ss, x_ss, kr_ss, vr_ss, a_ss, p_ss, t_ss, k_rs, v_rs, q_rs, x_rs, kr_rs, vr_rs,
    a_rs, t1_rs, t3_rs, p_rs,
):
    p = lax.axis_index("seq")
    t = lax.axis_index("tp")
    groups = n // heads
    head = p // groups
    group = p % groups
    tokens = img_ref.shape[1]
    text = txt_hbm.shape[1]
    share = text // groups
    plane_keys = heads * tokens
    early_keys = plane_keys + text
    scale = 1.0 / math.sqrt(HD)
    chunks = p_send.shape[0]
    width = p_send.shape[2]
    half = tokens // 2
    plane = largest_divisor(n)
    lines = n // plane
    inner = largest_divisor(plane)
    outer = plane // inner
    line = p // plane
    v = p % inner
    u = (p // inner) % outer
    near = plane % groups == 0 and groups % inner == 0 and inner % groups == 0
    by_head, by_group = Ring(head, heads), Ring(group, groups)
    by_line, by_u, by_v = Ring(line, lines), Ring(u, outer), Ring(v, inner)
    joined = 2 if by_head.paired and heads % 2 == 0 else heads
    pairs = heads // joined
    by_pair = Ring(head // joined, pairs)

    def on(core):
        return pl.when(t == core)

    def rows(first, count):
        return pl.ds(pl.multiple_of(first, count), count)

    def cols(h):
        return pl.ds(pl.multiple_of(h * HD, HD), HD)

    def plane_slot(j):
        return rows(j * tokens, tokens)

    def relay_slot(o, j):
        return pl.ds(pl.multiple_of(early_keys + ((o - 1) * heads + j) * tokens, tokens), tokens)

    def remote(src, dst, send, recv, seq, core):
        return pltpu.make_async_remote_copy(src, dst, send, recv, device_id={"seq": seq, "tp": core})

    def all_of(count, send, recv):
        if count <= k_all.shape[1]:
            block = k_all.at[0, pl.ds(0, count)]
        else:
            assert count * HD % w.shape[1] == 0
            block = w.at[pl.ds(0, count * HD // w.shape[1])]
        return remote(block, block, send, recv, p, 1 - t)

    barrier = pltpu.get_barrier_semaphore()

    def greet(seq, core):
        pl.semaphore_signal(barrier, inc=1, device_id={"seq": seq, "tp": core})

    def line_up(h):
        return h * groups + group

    def place(l, uu, vv):
        return l * plane + uu * inner + vv

    corners = [(i, k) for i in range(1, outer) for k in range(1, inner)]
    greet(p, 1 - t)
    if near:
        over(1, heads, lambda o: greet(line_up(by_head.to(heads - o)), WORK))
        over(1, groups, lambda o: greet(head * groups + by_group.to(o), WORK))
        for i, k in corners:
            greet(place(line, by_u.to(i), by_v.to(k)), WORK)

        @on(WORK)
        def _():
            over(1, heads, lambda o: greet(line_up(by_head.to(heads - o)), HELP))

        greetings = {WORK: 2 * (heads - 1 + groups - 1 + len(corners)) + 1, HELP: heads}
    else:
        over(1, n, lambda o: greet((p + o) % n, WORK))
        over(1, n, lambda o: greet((p + o) % n, HELP))
        greetings = {WORK: 2 * n - 1, HELP: 2 * n - 1}

    own_text = rows(group * share, share)
    text_keys = pl.ds(plane_keys, text)
    loads = [
        pltpu.make_async_copy(src, dst, load_sem.at[i])
        for i, (src, dst) in enumerate(
            (
                (frame_hbm, places.at[0]),
                (row_hbm, places.at[1]),
                (column_hbm, places.at[2]),
                (img_hbm, img_ref),
                (txt_hbm.at[0, own_text, cols(head)], txt_q.at[WORK]),
                (txt_hbm.at[1, :, cols(head)], k_all.at[WORK, text_keys]),
                (txt_hbm.at[2, :, cols(head)], v_all.at[WORK, text_keys]),
                (w_hbm, w),
                (res_hbm, res),
                (bias_hbm, bias),
                (gate_hbm, gate),
            )
        )
    ]
    for load in loads:
        load.start()

    diagonal = lax.broadcasted_iota(jnp.int32, (tokens, tokens), 0) == lax.broadcasted_iota(
        jnp.int32, (tokens, tokens), 1
    )
    channel = lax.broadcasted_iota(jnp.int32, (1, HD), 1)
    first = HD // 8
    second = (HD - first) // 2
    angles = jnp.zeros((tokens, HD), F32)
    for load in loads[:4]:
        load.wait()
    for part, (start, size) in enumerate(
        ((0, first), (first, second), (first + second, second))
    ):
        inside = (channel >= start) & (channel < start + size)
        pair = ((channel - start) // 2).astype(F32)
        rate = jnp.where(inside, jnp.exp2(pair * (-2.0 * ROPE_BASE_LOG2 / size)), 0.0)
        column = jnp.sum(
            jnp.where(diagonal, places[part].astype(F32), 0.0), axis=1, keepdims=True
        )
        angles = angles + column * rate
    even = lax.broadcasted_iota(jnp.int32, (tokens, HD), 1) % 2 == 0
    cosine = jnp.cos(angles)
    sine = jnp.where(even, -1.0, 1.0) * jnp.sin(angles)
    for which, dst in ((1, k_send), (0, q_send)):
        for h in range(heads):
            x = img_ref[which, :, h * HD : (h + 1) * HD].astype(F32)
            partner = jnp.where(even, pltpu.roll(x, HD - 1, 1), pltpu.roll(x, 1, 1))
            dst[h] = (x * cosine + partner * sine).astype(BF16)

    relayed = (groups - 1) * plane_keys

    def k_copy(o, h, core):
        return remote(k_send.at[h], k_all.at[core, plane_slot(head)], k_ss, k_rs.at[o], line_up(h), WORK)

    def v_copy(o, h, core):
        return remote(img_ref.at[2, :, cols(h)], v_all.at[core, plane_slot(head)], v_ss, v_rs.at[o], line_up(h), WORK)

    def q_copy(o, h, core):
        return remote(q_send.at[h], q_all.at[core, plane_slot(head)], q_ss, q_rs, line_up(h), WORK)

    def finish(count, sem):
        if count:
            all_of(count, sem, sem).wait_send()

    @on(HELP)
    def _():
        pl.semaphore_wait(barrier, greetings[HELP])
        for copy in (k_copy, v_copy, q_copy):
            for o in range(heads):
                copy(o, by_head.to(o), HELP).start()
        remote(txt_hbm.at[0, own_text, cols(head)], txt_q.at[HELP], x_ss, x_rs, p, WORK).start()
        remote(txt_hbm.at[1, :, cols(head)], k_all.at[HELP, text_keys], x_ss, x_rs, p, WORK).start()
        remote(txt_hbm.at[2, :, cols(head)], v_all.at[HELP, text_keys], x_ss, x_rs, p, WORK).start()

    def block(ref, s):
        return ref.at[rows((s % groups) * share, share), cols(s // groups)]

    @on(WORK)
    def _():
        k_all[WORK, plane_slot(head), :] = k_send[head]
        v_all[WORK, plane_slot(head), :] = img_ref[2, :, cols(head)]
        q_all[WORK, plane_slot(head), :] = q_send[head]
        pl.semaphore_wait(barrier, greetings[WORK])
        for copy in (k_copy, v_copy, q_copy):
            for o in range(1, heads):
                copy(o, by_head.to(o), WORK).start()

        def pass_on(data, got, send, recv):
            for o in range(heads):
                j = by_head.source(o)
                all_of((2 if o else 1) * tokens, send, got.at[o]).wait_recv()

                def one(i, j=j):
                    remote(
                        data.at[:, plane_slot(j)], data.at[:, relay_slot(i, j)], send, recv,
                        head * groups + by_group.to(i), WORK,
                    ).start()

                over(1, groups, one)

        pass_on(k_all, k_rs, kr_ss, kr_rs)
        pass_on(v_all, v_rs, vr_ss, vr_rs)
        for load in loads[4:7]:
            load.wait()
        all_of(share + 2 * text, x_ss, x_rs).wait_recv()
        length = len_ref[0]

        def scores_of(queries, core, start, count):
            return lax.dot_general(
                queries, k_all[core, pl.ds(start, count), :], (((1,), (1,)), ((), ())), preferred_element_type=F32
            )

        def early_scores(queries, core):
            scores = scores_of(queries, core, 0, early_keys)
            live = lax.broadcasted_iota(jnp.int32, scores.shape, 1) < plane_keys + length
            return jnp.where(live, scores, NEG_LARGE)

        def weigh(queries, core, scores):
            peak = jnp.max(scores, axis=1, keepdims=True)
            parts = [scores]
            if relayed:
                parts.append(scores_of(queries, core, early_keys, relayed))
                peak = jnp.maximum(peak, jnp.max(parts[1], axis=1, keepdims=True))
            live = lax.broadcasted_iota(jnp.int32, scores.shape, 1) < plane_keys + length
            weights = [jnp.exp((part - peak) * scale) for part in parts]
            weights[0] = jnp.where(live, weights[0], 0.0)
            whole = sum(jnp.sum(part, axis=1, keepdims=True) for part in weights)
            return [part.astype(BF16) for part in weights], whole

        def blend(core, weights, whole):
            mixed = jnp.dot(weights[0], v_all[core, pl.ds(0, early_keys), :], preferred_element_type=F32)
            if relayed:
                mixed = mixed + jnp.dot(
                    weights[1], v_all[core, pl.ds(early_keys, relayed), :], preferred_element_type=F32
                )
            return mixed / whole

        cores = (HELP, WORK)
        text_scores = [early_scores(txt_q[core], core) for core in cores]
        if relayed:
            all_of(2 * relayed, kr_ss, kr_rs).wait_recv()
        text_weights = [weigh(txt_q[core], core, text_scores[core]) for core in cores]
        if relayed:
            all_of(2 * relayed, vr_ss, vr_rs).wait_recv()
        for core in cores:
            done = blend(core, *text_weights[core])
            text_row = lax.broadcasted_iota(jnp.int32, done.shape, 0) + group * share
            done = jnp.where(text_row < length, done, 0.0).astype(BF16)
            t_send[core] = done
            if core == WORK:
                txt_out[own_text, cols(head)] = done
        held = {HELP: stage, WORK: txt_out}
        for o in range(1, lines):
            for core in cores:
                remote(
                    t_send.at[core], block(held[core], p), t_ss.at[0], t1_rs.at[o, core], place(by_line.to(o), u, v), WORK
                ).start()

        members = [(i, k) for i in range(outer) for k in range(inner) if i or k]

        def cross(l, core, own):
            s = place(l, u, v)
            source = t_send.at[core] if own else block(held[core], s)
            for i, k in members:
                remote(
                    source, block(txt_out, s), t_ss.at[1 + core], t3_rs, place(line, by_u.to(i), by_v.to(k)), core
                ).start()
            if core == HELP:
                remote(source, block(txt_out, s), t_ss.at[1 + core], t3_rs, p, core).start()

        for core in cores:
            cross(line, core, True)
        all_of((2 * heads - 1) * tokens, q_ss, q_rs).wait_recv()
        image_weights = [weigh(q_all[core], core, early_scores(q_all[core], core)) for core in cores]
        for core in cores:
            a_send[core] = blend(core, *image_weights[core]).astype(BF16)
        home[:, cols(head)] = a_send[WORK, plane_slot(head), :]
        for o in range(heads):
            j = by_head.to(o)
            for core in cores:
                if o or core == HELP:
                    remote(
                        a_send.at[core, plane_slot(j)], home.at[:, cols(head)], a_ss, a_rs.at[o // joined], line_up(j), core
                    ).start()
        for o in range(1, lines):
            for core in cores:
                all_of(share, t_ss.at[0], t1_rs.at[o, core]).wait_recv()
                cross(by_line.source(o), core, False)

    def project(o):
        @on(HELP)
        def _():
            all_of(joined * tokens, a_ss, a_rs.at[o]).wait_recv()

        @on(WORK)
        def _():
            count = joined * tokens - (tokens if o == 0 else 0)
            if count:
                all_of(count, a_ss, a_rs.at[o]).wait_recv()

        at = rows(by_pair.to(o) * joined * HD, joined * HD)
        return [
            jnp.dot(home[:, at], w[at, c * width : (c + 1) * width], preferred_element_type=F32)
            for c in range(chunks)
        ]

    def p_copy(c):
        return remote(p_send.at[c], p_recv.at[c], p_ss, p_rs.at[c], p, 1 - t)

    for load in loads[7:]:
        load.wait()
    for o in range(pairs - 1):
        for c, part in enumerate(project(o)):
            at = slice(c * width, (c + 1) * width)
            total[:, at] = part if o == 0 else total[:, at] + part
    last = project(pairs - 1)
    mine = []
    for c in range(chunks):
        at = slice(c * width, (c + 1) * width)
        part = last[c] if pairs == 1 else total[:, at] + last[c]
        top, bottom = part[:half], part[half:]
        p_send[c] = jnp.where(t == 0, bottom, top).astype(BF16)
        p_copy(c).start()
        mine.append(jnp.where(t == 0, top, bottom))
    for c in range(chunks):
        at = slice(c * width, (c + 1) * width)
        p_copy(c).wait_recv()
        projected = mine[c] + p_recv[c].astype(F32)
        out_ref[:, at] = (
            res[:, at].astype(F32) + gate[:, at] * (projected + bias[:, at])
        ).astype(BF16)

    @on(HELP)
    def _():
        for load in loads[4:7]:
            load.wait()
        remote(txt_out, txt_out, t_ss.at[0], t3_rs, p, 1 - t).wait_recv()
        for sem in (k_ss, v_ss, q_ss):
            finish(heads * tokens, sem)
        finish(share + 2 * text, x_ss)

    @on(WORK)
    def _():
        if plane > 1:
            all_of(lines * (plane - 1) * share, t_ss.at[0], t3_rs).wait_recv()
        for sem in (k_ss, v_ss, q_ss):
            finish((heads - 1) * tokens, sem)
        finish((2 * heads - 1) * tokens, a_ss)
        finish(2 * relayed, kr_ss)
        finish(2 * relayed, vr_ss)
        finish(2 * (lines - 1) * share, t_ss.at[0])
        remote(txt_out, txt_out, t_ss.at[1 + HELP], t3_rs, p, 1 - t).wait_send()
        finish(lines * (plane - 1) * share, t_ss.at[1 + WORK])

    remote(p_send, p_recv, p_ss, p_rs.at[0], p, 1 - t).wait_send()


def store(img, txt, img_out, txt_out, store_sem):
    stores = [
        pltpu.make_async_copy(a, b.at[0], store_sem.at[i]) for i, (a, b) in enumerate(((txt, txt_out), (img, img_out)))
    ]
    for put in stores:
        put.start()
    for put in stores:
        put.wait()


def shards(img_qkv, txt_qkv, frame_index, row_index, column_index, txt_len, residual, w_proj, proj_bias, gate):
    tokens = img_qkv.shape[1]
    channels = img_qkv.shape[3]
    heads = channels // HD
    n = lax.axis_size("seq")
    groups = n // heads
    text = txt_qkv.shape[1]
    share = text // groups
    lines = n // largest_divisor(n)
    pairs = max(heads // 2, 1)
    model = w_proj.shape[1]
    half = residual.shape[1]
    chunks = 4
    img = img_qkv[0].transpose(1, 0, 2)
    txt = txt_qkv[0].transpose(1, 0, 2)
    hbm = pl.BlockSpec(memory_space=pltpu.HBM)
    vmem = pl.BlockSpec(memory_space=pltpu.VMEM)
    dma = pltpu.SemaphoreType.DMA
    done = pl.pallas_call(
        functools.partial(kernel, n, heads),
        out_shape=(pltpu.VMEM((half, model), BF16), pltpu.VMEM((text, channels), BF16)),
        in_specs=[hbm] * 5 + [pl.BlockSpec(memory_space=pltpu.SMEM)] + [hbm] * 4,
        out_specs=(vmem, vmem),
        scratch_shapes=[
            pltpu.VMEM((3, tokens, channels), BF16),
            pltpu.VMEM((2, share, HD), BF16),
            pltpu.VMEM((3, 1, tokens), jnp.int32),
            pltpu.VMEM((heads, tokens, HD), BF16),
            pltpu.VMEM((heads, tokens, HD), BF16),
            pltpu.VMEM((2, heads * tokens, HD), BF16),
            pltpu.VMEM((2, n * tokens + text, HD), BF16),
            pltpu.VMEM((2, n * tokens + text, HD), BF16),
            pltpu.VMEM((2, heads * tokens, HD), BF16),
            pltpu.VMEM((tokens, channels), BF16),
            pltpu.VMEM((2, share, HD), BF16),
            pltpu.VMEM((text, channels), BF16),
            pltpu.VMEM(w_proj.shape, BF16),
            pltpu.VMEM((half, model), BF16),
            pltpu.VMEM((1, model), F32),
            pltpu.VMEM((1, model), F32),
            pltpu.VMEM((tokens, model), F32),
            pltpu.VMEM((chunks, half, model // chunks), BF16),
            pltpu.VMEM((chunks, half, model // chunks), BF16),
            dma((LOADS,)),
            dma, dma, dma, dma, dma, dma, dma, dma, dma((3,)),
            dma((heads,)), dma((heads,)), dma, dma, dma, dma,
            dma((pairs,)), dma((lines, 2)), dma, dma((chunks,)),
        ],
        compiler_params=pltpu.CompilerParams(
            collective_id=0, has_side_effects=True, vmem_limit_bytes=60000000
        ),
    )(
        img, txt, frame_index, row_index, column_index, txt_len, residual[0], w_proj,
        proj_bias[None], gate[None],
    )
    out, txt_out = (pltpu.with_memory_space_constraint(x, pltpu.VMEM) for x in done)
    return pl.pallas_call(
        store,
        out_shape=(
            jax.ShapeDtypeStruct((1,) + out.shape, BF16),
            jax.ShapeDtypeStruct((1,) + txt_out.shape, BF16),
        ),
        in_specs=[vmem, vmem],
        out_specs=(hbm, hbm),
        scratch_shapes=[dma((2,))],
        compiler_params=pltpu.CompilerParams(vmem_limit_bytes=8000000),
    )(out, txt_out)


def solution(mesh):
    in_specs = (
        P(None, "seq", None, "tp"),
        P(None, None, None, "tp"),
        P(None, "seq"),
        P(None, "seq"),
        P(None, "seq"),
        P(),
        P(None, ("seq", "tp"), None),
        P("tp", None),
        P(),
        P(),
    )
    out_specs = (P(None, ("seq", "tp"), None), P(None, None, "tp"))
    return jax.shard_map(shards, mesh=mesh, in_specs=in_specs, out_specs=out_specs, check_vma=False)
```

```python
import functools
import math

import jax
import jax.numpy as jnp
from jax import lax
from jax.experimental import pallas as pl
from jax.experimental.pallas import tpu as pltpu
from jax.sharding import PartitionSpec as P

HD = 128
ROPE_BASE_LOG2 = 8.0
NEG_LARGE = -1e30
F32 = jnp.float32
BF16 = jnp.bfloat16
LOADS = 6
HELP, WORK = 0, 1


def largest_divisor(n):
    best = 1
    for d in range(1, n + 1):
        if n % d == 0 and d * d <= n:
            best = d
    return best


def over(start, count, f):
    if count - start <= 8:
        for o in range(start, count):
            f(o)
    else:
        lax.fori_loop(start, count, lambda o, c: (f(o), c)[1], 0)


class Ring:
    def __init__(self, index, count):
        self.index, self.count = index, count
        self.paired = count & (count - 1) == 0
        self.flips = []
        if self.paired:
            bit = 1
            while bit < count:
                self.flips.append((bit, (1 - 2 * ((index // bit) % 2)) * bit))
                bit *= 2

    def meet(self, o, sign):
        if not self.paired:
            return (self.index + sign * o + self.count) % self.count
        total = self.index
        for bit, flip in self.flips:
            if isinstance(o, int):
                total = total + flip if o & bit else total
            else:
                total = total + flip * ((o // bit) % 2)
        return total

    def to(self, o):
        return self.meet(o, 1)

    def source(self, o):
        return self.meet(o, -1)


def kernel(
    n, heads, img_hbm, txt_hbm, frame_hbm, row_hbm, column_hbm, len_ref, res_hbm, w_hbm, bias_hbm, gate_hbm,
    out_ref, txt_out,
    img_ref, txt_q, places, q_send, k_send, q_all, k_all, v_all, a_send, home, t_send, stage, w, res, scales, total,
    p_send, p_recv, load_sem, out_ss, relay_ss, p_ss, t_ss, k_rs, v_rs, q_rs, x_rs, kr_rs, vr_rs,
    a_rs, t1_rs, t3_rs, p_rs,
):
    p = lax.axis_index("seq")
    t = lax.axis_index("tp")
    groups = n // heads
    head = p // groups
    group = p % groups
    tokens = img_ref.shape[1]
    text = txt_hbm.shape[1]
    share = text // groups
    plane_keys = heads * tokens
    early_keys = plane_keys + text
    scale = 1.0 / math.sqrt(HD)
    chunks = p_send.shape[0]
    width = p_send.shape[2]
    half = tokens // 2
    plane = largest_divisor(n)
    lines = n // plane
    inner = largest_divisor(plane)
    outer = plane // inner
    line = p // plane
    v = p % inner
    u = (p // inner) % outer
    near = plane % groups == 0 and groups % inner == 0 and inner % groups == 0
    by_head, by_group = Ring(head, heads), Ring(group, groups)
    by_line, by_u, by_v = Ring(line, lines), Ring(u, outer), Ring(v, inner)
    joined = 2 if by_head.paired and heads % 2 == 0 else heads
    pairs = heads // joined
    by_pair = Ring(head // joined, pairs)

    def on(core):
        return pl.when(t == core)

    def rows(first, count):
        return pl.ds(pl.multiple_of(first, count), count)

    def cols(h):
        return pl.ds(pl.multiple_of(h * HD, HD), HD)

    def plane_slot(j):
        return rows(j * tokens, tokens)

    def relay_slot(o, j):
        return pl.ds(pl.multiple_of(early_keys + ((o - 1) * heads + j) * tokens, tokens), tokens)

    def remote(src, dst, send, recv, seq, core):
        return pltpu.make_async_remote_copy(src, dst, send, recv, device_id={"seq": seq, "tp": core})

    def all_of(count, send, recv):
        if count <= k_all.shape[1]:
            block = k_all.at[0, pl.ds(0, count)]
        elif count <= 2 * k_all.shape[1] and count % 2 == 0:
            block = k_all.at[:, pl.ds(0, count // 2)]
        else:
            assert count * HD % w.shape[1] == 0
            block = w.at[pl.ds(0, count * HD // w.shape[1])]
        return remote(block, block, send, recv, p, 1 - t)

    barrier = pltpu.get_barrier_semaphore()

    def greet(seq, core):
        pl.semaphore_signal(barrier, inc=1, device_id={"seq": seq, "tp": core})

    def line_up(h):
        return h * groups + group

    def place(l, uu, vv):
        return l * plane + uu * inner + vv

    corners = [(i, k) for i in range(1, outer) for k in range(1, inner)]
    greet(p, 1 - t)
    if near:
        over(1, heads, lambda o: greet(line_up(by_head.to(heads - o)), WORK))
        over(1, groups, lambda o: greet(head * groups + by_group.to(o), WORK))
        for i, k in corners:
            greet(place(line, by_u.to(i), by_v.to(k)), WORK)

        @on(WORK)
        def _():
            over(1, heads, lambda o: greet(line_up(by_head.to(heads - o)), HELP))

        greetings = {WORK: 2 * (heads - 1 + groups - 1 + len(corners)) + 1, HELP: heads}
    else:
        over(1, n, lambda o: greet((p + o) % n, WORK))
        over(1, n, lambda o: greet((p + o) % n, HELP))
        greetings = {WORK: 2 * n - 1, HELP: 2 * n - 1}

    own_text = rows(group * share, share)
    text_keys = pl.ds(plane_keys, text)
    loads = [
        pltpu.make_async_copy(src, dst, load_sem.at[i])
        for i, src, dst in (
            (0, frame_hbm, places.at[0]),
            (0, row_hbm, places.at[1]),
            (0, column_hbm, places.at[2]),
            (1, img_hbm, img_ref),
            (2, txt_hbm.at[0, own_text, cols(head)], txt_q.at[WORK]),
            (2, txt_hbm.at[1, :, cols(head)], k_all.at[WORK, text_keys]),
            (2, txt_hbm.at[2, :, cols(head)], v_all.at[WORK, text_keys]),
            (3, w_hbm, w),
            (4, res_hbm, res),
            (5, bias_hbm, scales.at[0]),
            (5, gate_hbm, scales.at[1]),
        )
    ]

    def loaded(ref, i):
        pltpu.make_async_copy(ref, ref, load_sem.at[i]).wait()

    def loaded_text():
        loaded(k_all.at[WORK, pl.ds(0, share + 2 * text)], 2)

    for load in loads:
        load.start()

    diagonal = lax.broadcasted_iota(jnp.int32, (tokens, tokens), 0) == lax.broadcasted_iota(
        jnp.int32, (tokens, tokens), 1
    )
    channel = lax.broadcasted_iota(jnp.int32, (1, HD), 1)
    first = HD // 8
    second = (HD - first) // 2
    angles = jnp.zeros((tokens, HD), F32)
    loaded(places, 0)
    loaded(img_ref, 1)
    for part, (start, size) in enumerate(
        ((0, first), (first, second), (first + second, second))
    ):
        inside = (channel >= start) & (channel < start + size)
        pair = ((channel - start) // 2).astype(F32)
        rate = jnp.where(inside, jnp.exp2(pair * (-2.0 * ROPE_BASE_LOG2 / size)), 0.0)
        column = jnp.sum(
            jnp.where(diagonal, places[part].astype(F32), 0.0), axis=1, keepdims=True
        )
        angles = angles + column * rate
    even = lax.broadcasted_iota(jnp.int32, (tokens, HD), 1) % 2 == 0
    cosine = jnp.cos(angles)
    sine = jnp.where(even, -1.0, 1.0) * jnp.sin(angles)
    for which, dst in ((1, k_send), (0, q_send)):
        for h in range(heads):
            x = img_ref[which, :, h * HD : (h + 1) * HD].astype(F32)
            partner = jnp.where(even, pltpu.roll(x, HD - 1, 1), pltpu.roll(x, 1, 1))
            dst[h] = (x * cosine + partner * sine).astype(BF16)

    relayed = (groups - 1) * plane_keys

    def k_copy(o, h, core):
        return remote(k_send.at[h], k_all.at[core, plane_slot(head)], out_ss, k_rs.at[o], line_up(h), WORK)

    def v_copy(o, h, core):
        return remote(img_ref.at[2, :, cols(h)], v_all.at[core, plane_slot(head)], out_ss, v_rs.at[o], line_up(h), WORK)

    def q_copy(o, h, core):
        return remote(q_send.at[h], q_all.at[core, plane_slot(head)], out_ss, q_rs, line_up(h), WORK)

    def finish(count, sem):
        if count:
            all_of(count, sem, sem).wait_send()

    @on(HELP)
    def _():
        pl.semaphore_wait(barrier, greetings[HELP])
        for copy in (k_copy, v_copy, q_copy):
            for o in range(heads):
                copy(o, by_head.to(o), HELP).start()
        remote(txt_hbm.at[0, own_text, cols(head)], txt_q.at[HELP], out_ss, x_rs, p, WORK).start()
        remote(txt_hbm.at[1, :, cols(head)], k_all.at[HELP, text_keys], out_ss, x_rs, p, WORK).start()
        remote(txt_hbm.at[2, :, cols(head)], v_all.at[HELP, text_keys], out_ss, x_rs, p, WORK).start()

    def block(ref, s):
        return ref.at[rows((s % groups) * share, share), cols(s // groups)]

    @on(WORK)
    def _():
        k_all[WORK, plane_slot(head), :] = k_send[head]
        v_all[WORK, plane_slot(head), :] = img_ref[2, :, cols(head)]
        q_all[WORK, plane_slot(head), :] = q_send[head]
        pl.semaphore_wait(barrier, greetings[WORK])
        for copy in (k_copy, v_copy, q_copy):
            for o in range(1, heads):
                copy(o, by_head.to(o), WORK).start()

        def pass_on(data, got, send, recv):
            for o in range(heads):
                j = by_head.source(o)
                all_of((2 if o else 1) * tokens, send, got.at[o]).wait_recv()

                def one(i, j=j):
                    remote(
                        data.at[:, plane_slot(j)], data.at[:, relay_slot(i, j)], send, recv,
                        head * groups + by_group.to(i), WORK,
                    ).start()

                over(1, groups, one)

        pass_on(k_all, k_rs, relay_ss, kr_rs)
        pass_on(v_all, v_rs, relay_ss, vr_rs)
        loaded_text()
        all_of(share + 2 * text, out_ss, x_rs).wait_recv()
        length = len_ref[0]

        def scores_of(queries, core, start, count):
            return lax.dot_general(
                queries, k_all[core, pl.ds(start, count), :], (((1,), (1,)), ((), ())), preferred_element_type=F32
            )

        def early_scores(queries, core):
            scores = scores_of(queries, core, 0, early_keys)
            live = lax.broadcasted_iota(jnp.int32, scores.shape, 1) < plane_keys + length
            return jnp.where(live, scores, NEG_LARGE)

        def weigh(queries, core, scores):
            peak = jnp.max(scores, axis=1, keepdims=True)
            parts = [scores]
            if relayed:
                parts.append(scores_of(queries, core, early_keys, relayed))
                peak = jnp.maximum(peak, jnp.max(parts[1], axis=1, keepdims=True))
            live = lax.broadcasted_iota(jnp.int32, scores.shape, 1) < plane_keys + length
            weights = [jnp.exp((part - peak) * scale) for part in parts]
            weights[0] = jnp.where(live, weights[0], 0.0)
            whole = sum(jnp.sum(part, axis=1, keepdims=True) for part in weights)
            return [part.astype(BF16) for part in weights], whole

        def blend(core, weights, whole):
            mixed = jnp.dot(weights[0], v_all[core, pl.ds(0, early_keys), :], preferred_element_type=F32)
            if relayed:
                mixed = mixed + jnp.dot(
                    weights[1], v_all[core, pl.ds(early_keys, relayed), :], preferred_element_type=F32
                )
            return mixed / whole

        cores = (HELP, WORK)
        text_scores = [early_scores(txt_q[core], core) for core in cores]
        if relayed:
            all_of(2 * relayed, relay_ss, kr_rs).wait_recv()
        text_weights = [weigh(txt_q[core], core, text_scores[core]) for core in cores]
        if relayed:
            all_of(2 * relayed, relay_ss, vr_rs).wait_recv()
        for core in cores:
            done = blend(core, *text_weights[core])
            text_row = lax.broadcasted_iota(jnp.int32, done.shape, 0) + group * share
            done = jnp.where(text_row < length, done, 0.0).astype(BF16)
            t_send[core] = done
            if core == WORK:
                txt_out[own_text, cols(head)] = done
        held = {HELP: stage, WORK: txt_out}
        for o in range(1, lines):
            for core in cores:
                remote(
                    t_send.at[core], block(held[core], p), t_ss.at[0], t1_rs.at[o - 1, core], place(by_line.to(o), u, v), WORK
                ).start()

        members = [(i, k) for i in range(outer) for k in range(inner) if i or k]

        def cross(l, core, own):
            s = place(l, u, v)
            source = t_send.at[core] if own else block(held[core], s)
            for i, k in members:
                remote(
                    source, block(txt_out, s), t_ss.at[1 + core], t3_rs, place(line, by_u.to(i), by_v.to(k)), core
                ).start()
            if core == HELP:
                remote(source, block(txt_out, s), t_ss.at[1 + core], t3_rs, p, core).start()

        for core in cores:
            cross(line, core, True)
        all_of((2 * heads - 1) * tokens, out_ss, q_rs).wait_recv()
        image_weights = [weigh(q_all[core], core, early_scores(q_all[core], core)) for core in cores]
        for core in cores:
            a_send[core] = blend(core, *image_weights[core]).astype(BF16)
        home[:, cols(head)] = a_send[WORK, plane_slot(head), :]
        for o in range(heads):
            j = by_head.to(o)
            for core in cores:
                if o or core == HELP:
                    remote(
                        a_send.at[core, plane_slot(j)], home.at[:, cols(head)], out_ss, a_rs.at[o // joined], line_up(j), core
                    ).start()
        for o in range(1, lines):
            for core in cores:
                all_of(share, t_ss.at[0], t1_rs.at[o - 1, core]).wait_recv()
                cross(by_line.source(o), core, False)

    def project(o):
        @on(HELP)
        def _():
            all_of(joined * tokens, out_ss, a_rs.at[o]).wait_recv()

        @on(WORK)
        def _():
            count = joined * tokens - (tokens if o == 0 else 0)
            if count:
                all_of(count, out_ss, a_rs.at[o]).wait_recv()

        at = rows(by_pair.to(o) * joined * HD, joined * HD)
        return [
            jnp.dot(home[:, at], w[at, c * width : (c + 1) * width], preferred_element_type=F32)
            for c in range(chunks)
        ]

    def p_copy(c):
        return remote(p_send.at[c], p_recv.at[c], p_ss, p_rs.at[c], p, 1 - t)

    loaded(w, 3)
    loaded(res, 4)
    loaded(scales, 5)
    for o in range(pairs - 1):
        for c, part in enumerate(project(o)):
            at = slice(c * width, (c + 1) * width)
            total[:, at] = part if o == 0 else total[:, at] + part
    last = project(pairs - 1)
    mine = []
    for c in range(chunks):
        at = slice(c * width, (c + 1) * width)
        part = last[c] if pairs == 1 else total[:, at] + last[c]
        top, bottom = part[:half], part[half:]
        p_send[c] = jnp.where(t == 0, bottom, top).astype(BF16)
        p_copy(c).start()
        mine.append(jnp.where(t == 0, top, bottom))
    for c in range(chunks):
        at = slice(c * width, (c + 1) * width)
        p_copy(c).wait_recv()
        projected = mine[c] + p_recv[c].astype(F32)
        out_ref[:, at] = (
            res[:, at].astype(F32) + scales[1, :, at] * (projected + scales[0, :, at])
        ).astype(BF16)

    @on(HELP)
    def _():
        loaded_text()
        remote(txt_out, txt_out, t_ss.at[0], t3_rs, p, 1 - t).wait_recv()
        finish(3 * heads * tokens + share + 2 * text, out_ss)

    @on(WORK)
    def _():
        if plane > 1:
            all_of(lines * (plane - 1) * share, t_ss.at[0], t3_rs).wait_recv()
        finish((3 * (heads - 1) + 2 * heads - 1) * tokens, out_ss)
        finish(4 * relayed, relay_ss)
        finish(2 * (lines - 1) * share, t_ss.at[0])
        remote(txt_out, txt_out, t_ss.at[1 + HELP], t3_rs, p, 1 - t).wait_send()
        finish(lines * (plane - 1) * share, t_ss.at[1 + WORK])

    remote(p_send, p_recv, p_ss, p_rs.at[0], p, 1 - t).wait_send()


def store(img, txt, img_out, txt_out, store_sem):
    stores = [
        pltpu.make_async_copy(a, b.at[0], store_sem.at[i]) for i, (a, b) in enumerate(((txt, txt_out), (img, img_out)))
    ]
    for put in stores:
        put.start()
    for put in stores:
        put.wait()


def shards(img_qkv, txt_qkv, frame_index, row_index, column_index, txt_len, residual, w_proj, proj_bias, gate):
    tokens = img_qkv.shape[1]
    channels = img_qkv.shape[3]
    heads = channels // HD
    n = lax.axis_size("seq")
    groups = n // heads
    text = txt_qkv.shape[1]
    share = text // groups
    lines = n // largest_divisor(n)
    pairs = max(heads // 2, 1)
    model = w_proj.shape[1]
    half = residual.shape[1]
    chunks = 2
    img = img_qkv[0].transpose(1, 0, 2)
    txt = txt_qkv[0].transpose(1, 0, 2)
    hbm = pl.BlockSpec(memory_space=pltpu.HBM)
    vmem = pl.BlockSpec(memory_space=pltpu.VMEM)
    dma = pltpu.SemaphoreType.DMA
    done = pl.pallas_call(
        functools.partial(kernel, n, heads),
        out_shape=(pltpu.VMEM((half, model), BF16), pltpu.VMEM((text, channels), BF16)),
        in_specs=[hbm] * 5 + [pl.BlockSpec(memory_space=pltpu.SMEM)] + [hbm] * 4,
        out_specs=(vmem, vmem),
        scratch_shapes=[
            pltpu.VMEM((3, tokens, channels), BF16),
            pltpu.VMEM((2, share, HD), BF16),
            pltpu.VMEM((3, 1, tokens), jnp.int32),
            pltpu.VMEM((heads, tokens, HD), BF16),
            pltpu.VMEM((heads, tokens, HD), BF16),
            pltpu.VMEM((2, heads * tokens, HD), BF16),
            pltpu.VMEM((2, n * tokens + text, HD), BF16),
            pltpu.VMEM((2, n * tokens + text, HD), BF16),
            pltpu.VMEM((2, heads * tokens, HD), BF16),
            pltpu.VMEM((tokens, channels), BF16),
            pltpu.VMEM((2, share, HD), BF16),
            pltpu.VMEM((text, channels), BF16),
            pltpu.VMEM(w_proj.shape, BF16),
            pltpu.VMEM((half, model), BF16),
            pltpu.VMEM((2, 1, model), F32),
            pltpu.VMEM((tokens, model), F32),
            pltpu.VMEM((chunks, half, model // chunks), BF16),
            pltpu.VMEM((chunks, half, model // chunks), BF16),
            dma((LOADS,)),
            dma, dma, dma, dma((3,)),
            dma((heads,)), dma((heads,)), dma, dma, dma, dma,
            dma((pairs,)), dma((max(lines - 1, 1), 2)), dma, dma((chunks,)),
        ],
        compiler_params=pltpu.CompilerParams(
            collective_id=0, has_side_effects=True, vmem_limit_bytes=60000000
        ),
    )(
        img, txt, frame_index, row_index, column_index, txt_len, residual[0], w_proj,
        proj_bias[None], gate[None],
    )
    out, txt_out = (pltpu.with_memory_space_constraint(x, pltpu.VMEM) for x in done)
    return pl.pallas_call(
        store,
        out_shape=(
            jax.ShapeDtypeStruct((1,) + out.shape, BF16),
            jax.ShapeDtypeStruct((1,) + txt_out.shape, BF16),
        ),
        in_specs=[vmem, vmem],
        out_specs=(hbm, hbm),
        scratch_shapes=[dma((2,))],
        compiler_params=pltpu.CompilerParams(vmem_limit_bytes=8000000),
    )(out, txt_out)


def solution(mesh):
    in_specs = (
        P(None, "seq", None, "tp"),
        P(None, None, None, "tp"),
        P(None, "seq"),
        P(None, "seq"),
        P(None, "seq"),
        P(),
        P(None, ("seq", "tp"), None),
        P("tp", None),
        P(),
        P(),
    )
    out_specs = (P(None, ("seq", "tp"), None), P(None, None, "tp"))
    return jax.shard_map(shards, mesh=mesh, in_specs=in_specs, out_specs=out_specs, check_vma=False)
```
